8 devices in a mesh: dp: 2 (over y, z), tp: 4 (over x, core).
Axes of the slice: x: 2, y: 2, z: 1, core: 2. Of those that a mesh axis runs over, the one named last changes fastest.
Arguments:
- x: bfloat16 [4096, 5120], P('dp'), parts along dimension 0
- w_gate: bfloat16 [5120, 16384], P(None, 'tp')
- w_up: bfloat16 [5120, 16384], P(None, 'tp')
- w_down: bfloat16 [16384, 5120], P('tp')
Outputs:
- output: bfloat16 [4096, 5120], P('dp'), parts along dimension 0
There are 2 independent parts. The reference program is written for one: setup_inputs(seed, part) draws one part's arguments, and reference() takes and returns one part's arrays. A program takes and returns all parts, laid end to end along the dimension named above; an argument that names none is the same for every part.
All inputs are finite; a program needn't handle non-finite values.
Results may differ from the reference program's by a relative error of at most 0.016.
Values are sent between devices in bfloat16 or wider.
A program may use at most 2 GiB of HBM per device.

```python
import jax
import jax.numpy as jnp

ROWS = 2048
D = 5120
FF = 16384


def setup_inputs(seed: int = 0, part: int = 0) -> dict:
    kx, kg, ku, kd = jax.random.split(jax.random.key(seed), 4)
    drawn = {
        "x": jax.random.normal(jax.random.fold_in(kx, part), (ROWS, D), jnp.float32),
        "w_gate": jax.random.normal(kg, (D, FF), jnp.float32) * D**-0.5,
        "w_up": jax.random.normal(ku, (D, FF), jnp.float32) * D**-0.5,
        "w_down": jax.random.normal(kd, (FF, D), jnp.float32) * FF**-0.5,
    }
    return {k: v.astype(jnp.bfloat16) for k, v in drawn.items()}


def reference(x, w_gate, w_up, w_down):
    gate = jnp.dot(x, w_gate, preferred_element_type=jnp.float32)
    up = jnp.dot(x, w_up, preferred_element_type=jnp.float32)
    hidden = (jax.nn.silu(gate) * up).astype(jnp.bfloat16)
    return jnp.dot(hidden, w_down, preferred_element_type=jnp.float32).astype(jnp.bfloat16)
```

```python
import functools

import jax
import jax.numpy as jnp
from jax import lax
from jax.experimental import pallas as pl
from jax.experimental.pallas import tpu as pltpu
from jax.sharding import PartitionSpec as P

TG = 512
TD = 1024
SLOTS = 3
BF16, F32 = jnp.bfloat16, jnp.float32


def kernel(chunks, x, wg, wu, wd, y, xb, hid, ring, own, snd, rcv, xs, xr, fin,
           x_sem, ring_sem, d2d_s, d2d_r, ici_s, ici_r, fin_l, fin_s, fin_r):
    n_gu, n_d = wg.shape[1] // TG, wd.shape[1] // TD
    depth, ff = x.shape[1], wg.shape[1]
    per = n_gu + n_d
    n_chunks = sum(c for c, _ in chunks)
    me = lax.axis_index("tp")
    core = lax.rem(me, 2)
    partner = {"tp": me + 1 - 2 * core}
    across = {"tp": lax.rem(me + 2, 4)}

    def gu_copies(slot, j):
        cols = pl.ds(pl.multiple_of(j * TG, TG), TG)
        return (
            pltpu.make_async_copy(wg.at[:, cols], ring.at[slot, :, pl.ds(0, TG)], ring_sem.at[slot, 0]),
            pltpu.make_async_copy(wu.at[:, cols], ring.at[slot, :, pl.ds(TG, TG)], ring_sem.at[slot, 1]),
        )

    def d_copy(slot, j):
        cols = pl.ds(pl.multiple_of(j * TD, TD), TD)
        return pltpu.make_async_copy(wd.at[:, cols], ring.at[slot, pl.ds(0, ff), :], ring_sem.at[slot, 0])

    def x_copy(rows, row0, q):
        quarter = rows // 4
        half = lax.rem(q // 2 + core, 2)
        at = pl.multiple_of(row0 + half * (rows // 2) + lax.rem(q, 2) * quarter, quarter)
        return pltpu.make_async_copy(
            x.at[pl.ds(at, quarter), :],
            xb.at[pl.ds(pl.multiple_of(q * quarter, quarter), quarter), :],
            x_sem.at[q],
        )

    def d2d_copy(h, s):
        return pltpu.make_async_remote_copy(
            snd.at[s, pl.ds(0, h), :], rcv.at[s, pl.ds(0, h), :], d2d_s.at[s], d2d_r.at[s],
            device_id=partner, device_id_type=pl.DeviceIdType.MESH)

    def ici_copy(h, p, t):
        tile = (p, pl.ds(0, h), pl.ds(pl.multiple_of(t * TD, TD), TD))
        return pltpu.make_async_remote_copy(
            xs.at[tile], xr.at[tile], ici_s.at[p, t], ici_r.at[p, t],
            device_id=across, device_id_type=pl.DeviceIdType.MESH)

    def fin_copies(h, row0, f, t, k):
        src = fin.at[f, pl.ds(0, h), :]
        dst = y.at[pl.ds(pl.multiple_of(row0 + core * h, h), h), pl.ds(pl.multiple_of(t * TD, TD), TD)]
        return (
            pltpu.make_async_copy(src, dst, fin_l.at[f]),
            pltpu.make_async_remote_copy(
                src, dst, fin_s.at[f], fin_r.at[k],
                device_id=partner, device_id_type=pl.DeviceIdType.MESH),
        )

    def reduce_tile(i, rows, t):
        h, s, p = rows // 2, lax.rem(i * n_d + t, 2), lax.rem(i, 2)
        d2d_copy(h, s).wait_recv()
        total = own[s, pl.ds(0, h), :] + rcv[s, pl.ds(0, h), :].astype(F32)
        xs[p, pl.ds(0, h), pl.ds(pl.multiple_of(t * TD, TD), TD)] = total.astype(BF16)
        ici_copy(h, p, t).start()

    def finish_tile(i, rows, row0, t, prior=None):
        h, p = rows // 2, lax.rem(i, 2)
        k = i * n_d + t
        f = lax.rem(k, 2)
        copy = ici_copy(h, p, t)
        copy.wait_send()
        copy.wait_recv()

        def release(r):
            local, remote = fin_copies(r // 2, 0, f, t, k)
            local.wait()
            remote.wait_send()

        if prior is None:
            pl.when(k >= 2)(lambda: release(rows))
        else:
            release(prior)
        tile = (p, pl.ds(0, h), pl.ds(pl.multiple_of(t * TD, TD), TD))
        fin[f, pl.ds(0, h), :] = (xs[tile].astype(F32) + xr[tile].astype(F32)).astype(BF16)
        for c in fin_copies(h, row0, f, t, k):
            c.start()

    def slot_of(i, s):
        return lax.rem(i * per + s, SLOTS)

    def chunk(i, rows, row0, before, last, following):
        h = rows // 2
        for q in range(4):
            x_copy(rows, row0, q).wait()
        row_before = row0 - before

        @pl.loop(0, n_gu)
        def _(j):
            slot = slot_of(i, j)
            for c in gu_copies(slot, j):
                c.wait()
            ahead = slot_of(i, j + SLOTS - 1)

            @pl.when(j + SLOTS - 1 < n_gu)
            def _():
                for c in gu_copies(ahead, j + SLOTS - 1):
                    c.start()

            @pl.when(j + SLOTS - 1 >= n_gu)
            def _():
                d_copy(ahead, j + SLOTS - 1 - n_gu).start()

            w = TG // 2
            for k in range(2):
                gate = jnp.dot(xb[pl.ds(0, rows), :], ring[slot, :, pl.ds(k * w, w)], preferred_element_type=F32)
                up = jnp.dot(xb[pl.ds(0, rows), :], ring[slot, :, pl.ds(TG + k * w, w)], preferred_element_type=F32)
                hid[pl.ds(0, rows), pl.ds(pl.multiple_of(j * TG + k * w, w), w)] = (
                    gate * jax.nn.sigmoid(gate) * up).astype(BF16)

            @pl.when((j == 0) & (i > 0))
            def _():
                reduce_tile(i - 1, before, n_d - 1)

            @pl.when((lax.rem(j, 2) == 1) & (i > 0))
            def _():
                finish_tile(i - 1, before, row_before, j // 2, None)

        @pl.loop(0, n_d)
        def _(j):
            slot = slot_of(i, n_gu + j)
            d_copy(slot, j).wait()
            ahead = slot_of(i, n_gu + j + SLOTS - 1)

            @pl.when(j + SLOTS - 1 < n_d)
            def _():
                d_copy(ahead, j + SLOTS - 1).start()

            if not last:
                more = (j + SLOTS - 1 >= n_d) & (i + 1 < n_chunks)

                @pl.when(more)
                def _():
                    for c in gu_copies(ahead, j + SLOTS - 1 - n_d):
                        c.start()

                @pl.when(j < 4)
                def _():
                    following(j).start()

            g = i * n_d + j
            s = lax.rem(g, 2)

            @pl.when(g >= 2)
            def _():
                @pl.when(j >= 2)
                def _():
                    d2d_copy(h, s).wait_send()

                @pl.when(j < 2)
                def _():
                    d2d_copy(before // 2, s).wait_send()

            w = TD // 2
            for k in range(2):
                cols = pl.ds(k * w, w)
                term = jnp.dot(hid[pl.ds(0, rows), :], ring[slot, pl.ds(0, ff), cols], preferred_element_type=F32)
                own[s, pl.ds(0, h), cols] = term[:h]
                snd[s, pl.ds(0, h), cols] = term[h:].astype(BF16)

            @pl.when((j == 1) & (i > 0))
            def _():
                finish_tile(i - 1, before, row_before, n_d - 1, None)

            @pl.when(j > 0)
            def _():
                reduce_tile(i, rows, j - 1)

            d2d_copy(h, s).start()

    plan, row = [], 0
    for count, rows in chunks:
        for _ in range(count):
            plan.append((rows, row))
            row += rows

    for q in range(4):
        x_copy(plan[0][0], 0, q).start()
    for j in range(SLOTS - 1):
        for c in gu_copies(j, j):
            c.start()

    barrier = pltpu.get_barrier_semaphore()
    for peer in (partner, across):
        pl.semaphore_signal(barrier, inc=1, device_id=peer, device_id_type=pl.DeviceIdType.MESH)
    pl.semaphore_wait(barrier, 2)

    @pl.loop(0, n_chunks)
    def _(i):
        rows = plan[0][0]
        row0 = pl.multiple_of(i * rows, rows)

        @pl.when(i + 1 < n_chunks)
        def _():
            pass

        chunk(i, rows, row0, rows, False, lambda q: x_copy(rows, lax.rem(i + 1, n_chunks) * rows, q))

    rows, row0 = plan[-1]
    i = n_chunks - 1
    for q in range(4):
        x_copy(rows, 0, q).wait()
    reduce_tile(i, rows, n_d - 1)
    for t in range(n_d):
        finish_tile(i, rows, row0, t, rows)
    for s in range(2):
        d2d_copy(rows // 2, s).wait_send()
        local, remote = fin_copies(rows // 2, 0, s, 0, 0)
        local.wait()
        remote.wait_send()
    for k in range(n_chunks * n_d):
        fin_copies(plan[k // n_d][0] // 2, 0, 0, 0, k)[1].wait_recv()


def solution(mesh):
    chunks = ((4, 512),)
    biggest = max(r for _, r in chunks)
    n_chunks = sum(c for c, _ in chunks)

    def step(x, w_gate, w_up, w_down):
        (rows, depth), ff, width = x.shape, w_gate.shape[1], w_down.shape[1]
        h, n_d = biggest // 2, width // TD
        dma = pltpu.SemaphoreType.DMA
        return pl.pallas_call(
            functools.partial(kernel, chunks),
            out_shape=jax.ShapeDtypeStruct((rows, width), BF16),
            in_specs=[pl.BlockSpec(memory_space=pl.ANY)] * 4,
            out_specs=pl.BlockSpec(memory_space=pl.ANY),
            scratch_shapes=[
                pltpu.VMEM((biggest, depth), BF16),
                pltpu.VMEM((biggest, ff), BF16),
                pltpu.VMEM((SLOTS, depth, 2 * TG), BF16),
                pltpu.VMEM((2, h, TD), F32),
                pltpu.VMEM((2, h, TD), BF16),
                pltpu.VMEM((2, h, TD), BF16),
                pltpu.VMEM((2, h, width), BF16),
                pltpu.VMEM((2, h, width), BF16),
                pltpu.VMEM((2, h, TD), BF16),
                dma((4,)), dma((SLOTS, 2)), dma((2,)), dma((2,)), dma((2, n_d)), dma((2, n_d)),
                dma((2,)), dma((2,)), dma((n_chunks * n_d,)),
            ],
            compiler_params=pltpu.CompilerParams(
                collective_id=0, has_side_effects=True, vmem_limit_bytes=66_900_000),
            cost_estimate=pl.CostEstimate(
                flops=6 * rows * depth * ff, bytes_accessed=4 * 3 * depth * ff * 2, transcendentals=rows * ff),
        )(x, w_gate, w_up, w_down)

    return jax.shard_map(
        step,
        mesh=mesh,
        in_specs=(P("dp", None), P(None, "tp"), P(None, "tp"), P("tp", None)),
        out_specs=P("dp", None),
        check_vma=False,
    )
```

```python
import functools

import jax
import jax.numpy as jnp
from jax import lax
from jax.experimental import pallas as pl
from jax.experimental.pallas import tpu as pltpu
from jax.sharding import PartitionSpec as P

CHUNKS = (512, 512, 448, 320, 256)
TG = 512
TD = 1024
SLOTS = 3
PIECES = 16
BF16, F32 = jnp.bfloat16, jnp.float32


def kernel(x, wg, wu, wd, y, xb, hid, ring, own, snd, rcv, xs0, xs1, xr0, xr1,
           x_sem, ring_sem, d2d_s, d2d_r, ici_s, ici_r, fin_l, fin_s, fin_r, credit):
    ff = wg.shape[1]
    n_gu, n_d = ff // TG, wd.shape[1] // TD
    per = n_gu + n_d
    last = len(CHUNKS) - 1
    first_row = [sum(CHUNKS[:i]) for i in range(len(CHUNKS))]
    xs, xr = (xs0, xs1), (xr0, xr1)
    me = lax.axis_index("tp")
    core = lax.rem(me, 2)
    partner = {"tp": me + 1 - 2 * core}
    across = {"tp": lax.rem(me + 2, 4)}
    remote = functools.partial(pltpu.make_async_remote_copy, device_id_type=pl.DeviceIdType.MESH)

    def block(j, width):
        return pl.ds(pl.multiple_of(j * width, width), width)

    def slot_of(i, s):
        return lax.rem(i * per + s, SLOTS)

    def g_copy(slot, j):
        return pltpu.make_async_copy(wg.at[:, block(j, TG)], ring.at[slot, :, pl.ds(0, TG)], ring_sem.at[slot, 0])

    def u_copy(slot, j):
        return pltpu.make_async_copy(wu.at[:, block(j, TG)], ring.at[slot, :, pl.ds(TG, TG)], ring_sem.at[slot, 1])

    def d_copy(slot, j):
        return pltpu.make_async_copy(wd.at[:, block(j, TD)], ring.at[slot, pl.ds(0, ff), :], ring_sem.at[slot, 0])

    def x_copy(i, q):
        quarter = CHUNKS[i] // 4
        half = lax.rem(q // 2 + core, 2)
        at = pl.multiple_of(first_row[i] + (half * 2 + lax.rem(q, 2)) * quarter, quarter & -quarter)
        return pltpu.make_async_copy(x.at[pl.ds(at, quarter), :], xb.at[block(q, quarter), :], x_sem.at[q])

    def d2d_copy(i, s):
        h = CHUNKS[i] // 2
        return remote(snd.at[s, pl.ds(0, h), :], rcv.at[s, pl.ds(0, h), :], d2d_s.at[s], d2d_r.at[s], device_id=partner)

    def ici_copy(i, t):
        tile = (pl.ds(0, CHUNKS[i] // 2), block(t, TD))
        return remote(xs[i % 2].at[tile], xr[i % 2].at[tile], ici_s.at[i % 2, t], ici_r.at[i % 2, t], device_id=across)

    def fin_refs(i, t):
        h = CHUNKS[i] // 2
        at = pl.multiple_of(first_row[i] + core * h, h & -h)
        return xs[i % 2].at[pl.ds(0, h), block(t, TD)], y.at[pl.ds(at, h), block(t, TD)]

    def fin_here(i, t):
        src, dst = fin_refs(i, t)
        return pltpu.make_async_copy(src, dst, fin_l.at[i % 2, t])

    def fin_there(i, t):
        src, dst = fin_refs(i, t)
        return remote(src, dst, fin_s.at[i % 2, t], fin_r.at[i * n_d + t], device_id=partner)

    def fin_left(i, t):
        fin_here(i, t).wait()
        fin_there(i, t).wait_send()

    def reduce_tile(i, t):
        h, s = CHUNKS[i] // 2, lax.rem(i * n_d + t, 2)
        d2d_copy(i, s).wait_recv()
        if i >= 2:
            fin_left(i - 2, t)
        total = own[s, pl.ds(0, h), :] + rcv[s, pl.ds(0, h), :].astype(F32)
        xs[i % 2][pl.ds(0, h), block(t, TD)] = total.astype(BF16)
        ici_copy(i, t).start()

    def finish_tile(i, t):
        copy = ici_copy(i, t)
        copy.wait_send()
        copy.wait_recv()
        tile = (pl.ds(0, CHUNKS[i] // 2), block(t, TD))
        total = xs[i % 2][tile].astype(F32) + xr[i % 2][tile].astype(F32)
        xs[i % 2][tile] = total.astype(BF16)
        fin_here(i, t).start()
        fin_there(i, t).start()

    for q in range(4):
        x_copy(0, q).start()
    g_copy(0, 0).start()
    u_copy(0, 0).start()

    barrier = pltpu.get_barrier_semaphore()
    for peer in (partner, across):
        pl.semaphore_signal(barrier, inc=1, device_id=peer, device_id_type=pl.DeviceIdType.MESH)
    pl.semaphore_wait(barrier, 2)

    for i, rows in enumerate(CHUNKS):
        h = rows // 2
        for q in range(4):
            x_copy(i, q).wait()

        @pl.loop(0, n_gu)
        def _(j):
            slot, ahead, nxt = slot_of(i, j), slot_of(i, j + SLOTS - 1), j + SLOTS - 1
            g_copy(slot, j).wait()
            u_copy(slot, j).wait()

            if i == 0:

                @pl.when(j == 0)
                def _():
                    for early in range(1, SLOTS - 1):
                        g_copy(early, early).start()
                        u_copy(early, early).start()

            @pl.when(nxt < n_gu)
            def _():
                g_copy(ahead, nxt).start()
                u_copy(ahead, nxt).start()

            @pl.when(nxt >= n_gu)
            def _():
                d_copy(ahead, nxt - n_gu).start()

            w = TG // 2
            for k in range(2):
                gate = jnp.dot(xb[pl.ds(0, rows), :], ring[slot, :, pl.ds(k * w, w)], preferred_element_type=F32)
                up = jnp.dot(xb[pl.ds(0, rows), :], ring[slot, :, pl.ds(TG + k * w, w)], preferred_element_type=F32)
                act = gate * jax.nn.sigmoid(gate) * up
                hid[pl.ds(0, rows), pl.ds(pl.multiple_of(j * TG + k * w, w), w)] = act.astype(BF16)

            if i > 0:

                @pl.when(j == 0)
                def _():
                    reduce_tile(i - 1, n_d - 1)

            if i > 1:

                @pl.when(j < n_d)
                def _():
                    finish_tile(i - 2, j)

                @pl.when(j == n_d - 1)
                def _():
                    pl.semaphore_signal(credit, inc=1, device_id=across, device_id_type=pl.DeviceIdType.MESH)

        @pl.loop(0, n_d)
        def _(j):
            slot, ahead, nxt = slot_of(i, n_gu + j), slot_of(i, n_gu + j + SLOTS - 1), j + SLOTS - 1
            s = lax.rem(i * n_d + j, 2)
            d_copy(slot, j).wait()

            @pl.when(nxt < n_d)
            def _():
                d_copy(ahead, nxt).start()

            if i < last:

                @pl.when(nxt >= n_d)
                def _():
                    g_copy(ahead, nxt - n_d).start()
                    u_copy(ahead, nxt - n_d).start()

                @pl.when(j < 4)
                def _():
                    x_copy(i + 1, j).start()

            @pl.when(j >= 2)
            def _():
                d2d_copy(i, s).wait_send()

            if i > 0:

                @pl.when(j < 2)
                def _():
                    d2d_copy(i - 1, s).wait_send()

            w = TD // 2
            for k in range(2):
                term = jnp.dot(hid[pl.ds(0, rows), :], ring[slot, pl.ds(0, ff), pl.ds(k * w, w)], preferred_element_type=F32)
                own[s, pl.ds(0, h), pl.ds(k * w, w)] = term[:h]
                snd[s, pl.ds(0, h), pl.ds(k * w, w)] = term[h:].astype(BF16)

            if i > 1:

                @pl.when(j == 1)
                def _():
                    pl.semaphore_wait(credit, 1)

            @pl.when(j > 0)
            def _():
                reduce_tile(i, j - 1)

            d2d_copy(i, s).start()

    reduce_tile(last, n_d - 1)
    for i in (last - 1, last):
        for t in range(n_d):
            finish_tile(i, t)
    for s in range(2):
        d2d_copy(last, s).wait_send()
    for i in (last - 1, last):
        for t in range(n_d):
            fin_left(i, t)
    for i in range(len(CHUNKS)):
        for t in range(n_d):
            fin_there(i, t).wait_recv()


def copy_kernel(src, dst, buf, in_sem, out_sem):
    rows = src.shape[0] // PIECES

    def load(p):
        at = pl.ds(p * rows, rows)
        return pltpu.make_async_copy(src.at[at, :], buf.at[at, :], in_sem.at[p])

    def store(p):
        at = pl.ds(p * rows, rows)
        return pltpu.make_async_copy(buf.at[at, :], dst.at[at, :], out_sem.at[p])

    for p in range(PIECES):
        load(p).start()
    for p in range(PIECES):
        load(p).wait()
        store(p).start()
    for p in range(PIECES):
        store(p).wait()


def solution(mesh):
    def step(x, w_gate, w_up, w_down):
        (rows, depth), ff, width = x.shape, w_gate.shape[1], w_down.shape[1]
        big, n_d, n = max(CHUNKS), width // TD, len(CHUNKS)
        h = big // 2
        even, odd = max(CHUNKS[0::2]) // 2, max(CHUNKS[1::2]) // 2
        dma, vmem = pltpu.SemaphoreType.DMA, pltpu.VMEM
        anywhere = pl.BlockSpec(memory_space=pl.ANY)
        summed = pl.pallas_call(
            kernel,
            out_shape=jax.ShapeDtypeStruct((rows, width), BF16),
            in_specs=[anywhere] * 4,
            out_specs=anywhere,
            scratch_shapes=[
                vmem((big, depth), BF16),
                vmem((big, ff), BF16),
                vmem((SLOTS, depth, 2 * TG), BF16),
                vmem((2, h, TD), F32),
                vmem((2, h, TD), BF16),
                vmem((2, h, TD), BF16),
                vmem((even, width), BF16),
                vmem((odd, width), BF16),
                vmem((even, width), BF16),
                vmem((odd, width), BF16),
                dma((4,)), dma((SLOTS, 2)), dma((2,)), dma((2,)), dma((2, n_d)), dma((2, n_d)),
                dma((2, n_d)), dma((2, n_d)), dma((n * n_d,)),
                pltpu.SemaphoreType.REGULAR,
            ],
            compiler_params=pltpu.CompilerParams(
                collective_id=0, has_side_effects=True, vmem_limit_bytes=66_900_000),
            cost_estimate=pl.CostEstimate(
                flops=6 * rows * depth * ff, bytes_accessed=n * 6 * depth * ff, transcendentals=rows * ff),
        )(x, w_gate, w_up, w_down)
        return pl.pallas_call(
            copy_kernel,
            out_shape=jax.ShapeDtypeStruct((rows, width), BF16),
            in_specs=[anywhere],
            out_specs=anywhere,
            scratch_shapes=[vmem((rows, width), BF16), dma((PIECES,)), dma((PIECES,))],
            compiler_params=pltpu.CompilerParams(vmem_limit_bytes=40_000_000),
            cost_estimate=pl.CostEstimate(flops=0, bytes_accessed=4 * rows * width, transcendentals=0),
        )(summed)

    return jax.shard_map(
        step,
        mesh=mesh,
        in_specs=(P("dp", None), P(None, "tp"), P(None, "tp"), P("tp", None)),
        out_specs=P("dp", None),
        check_vma=False,
    )
```

```python
import functools

import jax
import jax.numpy as jnp
from jax import lax
from jax.experimental import pallas as pl
from jax.experimental.pallas import tpu as pltpu
from jax.sharding import PartitionSpec as P

CHUNKS = (512, 512, 448, 320, 256)
TG = 512
TD = 1024
SLOTS = 3
PIECES = 16
COPY_COST = 20_000_000_000
REST = 3
BF16, F32 = jnp.bfloat16, jnp.float32


def kernel(x, wg, wu, wd, y, rest, xb, hid, ring, own, snd, rcv, xs0, xs1, xr0, xr1,
           x_sem, ring_sem, d2d_s, d2d_r, ici_s, ici_r, fin_l, fin_s, fin_r, credit, rest_sem):
    ff = wg.shape[1]
    n_gu, n_d = ff // TG, wd.shape[1] // TD
    per = n_gu + n_d
    last = len(CHUNKS) - 1
    first_row = [sum(CHUNKS[:i]) for i in range(len(CHUNKS))]
    xs, xr = (xs0, xs1), (xr0, xr1)
    me = lax.axis_index("tp")
    core = lax.rem(me, 2)
    partner = {"tp": me + 1 - 2 * core}
    across = {"tp": lax.rem(me + 2, 4)}
    remote = functools.partial(pltpu.make_async_remote_copy, device_id_type=pl.DeviceIdType.MESH)

    def block(j, width):
        return pl.ds(pl.multiple_of(j * width, width), width)

    def slot_of(i, s):
        return lax.rem(i * per + s, SLOTS)

    def g_copy(slot, j):
        return pltpu.make_async_copy(wg.at[:, block(j, TG)], ring.at[slot, :, pl.ds(0, TG)], ring_sem.at[slot, 0])

    def u_copy(slot, j):
        return pltpu.make_async_copy(wu.at[:, block(j, TG)], ring.at[slot, :, pl.ds(TG, TG)], ring_sem.at[slot, 1])

    def d_copy(slot, j):
        return pltpu.make_async_copy(wd.at[:, block(j, TD)], ring.at[slot, pl.ds(0, ff), :], ring_sem.at[slot, 0])

    def x_copy(i, q):
        quarter = CHUNKS[i] // 4
        half = lax.rem(q // 2 + core, 2)
        at = pl.multiple_of(first_row[i] + (half * 2 + lax.rem(q, 2)) * quarter, quarter & -quarter)
        return pltpu.make_async_copy(x.at[pl.ds(at, quarter), :], xb.at[block(q, quarter), :], x_sem.at[q])

    def d2d_copy(i, s):
        h = CHUNKS[i] // 2
        return remote(snd.at[s, pl.ds(0, h), :], rcv.at[s, pl.ds(0, h), :], d2d_s.at[s], d2d_r.at[s], device_id=partner)

    def ici_copy(i, t):
        tile = (pl.ds(0, CHUNKS[i] // 2), block(t, TD))
        return remote(xs[i % 2].at[tile], xr[i % 2].at[tile], ici_s.at[i % 2, t], ici_r.at[i % 2, t], device_id=across)

    def fin_refs(i, t):
        h = CHUNKS[i] // 2
        at = pl.multiple_of(first_row[i] + core * h, h & -h)
        return xs[i % 2].at[pl.ds(0, h), block(t, TD)], y.at[pl.ds(at, h), block(t, TD)]

    def fin_here(i, t):
        src, dst = fin_refs(i, t)
        return pltpu.make_async_copy(src, dst, fin_l.at[i % 2, t])

    def fin_there(i, t):
        src, dst = fin_refs(i, t)
        return remote(src, dst, fin_s.at[i % 2, t], fin_r.at[i * n_d + t], device_id=partner)

    def fin_left(i, t):
        fin_here(i, t).wait()
        fin_there(i, t).wait_send()

    def rest_copy(t):
        k = t - (n_d - REST)
        src = xs[last % 2].at[pl.ds(0, CHUNKS[last] // 2), block(t, TD)]
        return pltpu.make_async_copy(src, rest.at[:, block(k, TD)], rest_sem.at[k])

    def reduce_tile(i, t):
        h, s = CHUNKS[i] // 2, lax.rem(i * n_d + t, 2)
        d2d_copy(i, s).wait_recv()
        if i >= 2:
            fin_left(i - 2, t)
        total = own[s, pl.ds(0, h), :] + rcv[s, pl.ds(0, h), :].astype(F32)
        xs[i % 2][pl.ds(0, h), block(t, TD)] = total.astype(BF16)
        if i < last:
            ici_copy(i, t).start()
        elif isinstance(t, int):
            rest_copy(t).start()
        else:
            pl.when(t < n_d - REST)(lambda: ici_copy(i, t).start())
            pl.when(t >= n_d - REST)(lambda: rest_copy(t).start())

    def finish_tile(i, t):
        copy = ici_copy(i, t)
        copy.wait_send()
        copy.wait_recv()
        tile = (pl.ds(0, CHUNKS[i] // 2), block(t, TD))
        total = xs[i % 2][tile].astype(F32) + xr[i % 2][tile].astype(F32)
        xs[i % 2][tile] = total.astype(BF16)
        fin_here(i, t).start()
        fin_there(i, t).start()

    for q in range(4):
        x_copy(0, q).start()
    g_copy(0, 0).start()
    u_copy(0, 0).start()

    barrier = pltpu.get_barrier_semaphore()
    for peer in (partner, across):
        pl.semaphore_signal(barrier, inc=1, device_id=peer, device_id_type=pl.DeviceIdType.MESH)
    pl.semaphore_wait(barrier, 2)

    for i, rows in enumerate(CHUNKS):
        h = rows // 2
        for q in range(4):
            x_copy(i, q).wait()

        @pl.loop(0, n_gu)
        def _(j):
            slot, ahead, nxt = slot_of(i, j), slot_of(i, j + SLOTS - 1), j + SLOTS - 1
            g_copy(slot, j).wait()
            u_copy(slot, j).wait()

            if i == 0:

                @pl.when(j == 0)
                def _():
                    for early in range(1, SLOTS - 1):
                        g_copy(early, early).start()
                        u_copy(early, early).start()

            @pl.when(nxt < n_gu)
            def _():
                g_copy(ahead, nxt).start()
                u_copy(ahead, nxt).start()

            @pl.when(nxt >= n_gu)
            def _():
                d_copy(ahead, nxt - n_gu).start()

            w = TG // 2
            for k in range(2):
                gate = jnp.dot(xb[pl.ds(0, rows), :], ring[slot, :, pl.ds(k * w, w)], preferred_element_type=F32)
                up = jnp.dot(xb[pl.ds(0, rows), :], ring[slot, :, pl.ds(TG + k * w, w)], preferred_element_type=F32)
                act = gate * jax.nn.sigmoid(gate) * up
                hid[pl.ds(0, rows), pl.ds(pl.multiple_of(j * TG + k * w, w), w)] = act.astype(BF16)

            if i > 0:

                @pl.when(j == 0)
                def _():
                    reduce_tile(i - 1, n_d - 1)

            if i > 1:

                @pl.when(j < n_d)
                def _():
                    finish_tile(i - 2, j)

                @pl.when(j == n_d - 1)
                def _():
                    pl.semaphore_signal(credit, inc=1, device_id=across, device_id_type=pl.DeviceIdType.MESH)

        @pl.loop(0, n_d)
        def _(j):
            slot, ahead, nxt = slot_of(i, n_gu + j), slot_of(i, n_gu + j + SLOTS - 1), j + SLOTS - 1
            s = lax.rem(i * n_d + j, 2)
            d_copy(slot, j).wait()

            @pl.when(nxt < n_d)
            def _():
                d_copy(ahead, nxt).start()

            if i < last:

                @pl.when(nxt >= n_d)
                def _():
                    g_copy(ahead, nxt - n_d).start()
                    u_copy(ahead, nxt - n_d).start()

                @pl.when(j < 4)
                def _():
                    x_copy(i + 1, j).start()

            @pl.when(j >= 2)
            def _():
                d2d_copy(i, s).wait_send()

            if i > 0:

                @pl.when(j < 2)
                def _():
                    d2d_copy(i - 1, s).wait_send()

            w = TD // 2
            for k in range(2):
                term = jnp.dot(hid[pl.ds(0, rows), :], ring[slot, pl.ds(0, ff), pl.ds(k * w, w)], preferred_element_type=F32)
                own[s, pl.ds(0, h), pl.ds(k * w, w)] = term[:h]
                snd[s, pl.ds(0, h), pl.ds(k * w, w)] = term[h:].astype(BF16)

            if i > 1:

                @pl.when(j == 1)
                def _():
                    pl.semaphore_wait(credit, 1)

            @pl.when(j > 0)
            def _():
                reduce_tile(i, j - 1)

            d2d_copy(i, s).start()

    reduce_tile(last, n_d - 1)
    def finished(i):
        return n_d if i < last else n_d - REST

    for i in (last - 1, last):
        for t in range(finished(i)):
            finish_tile(i, t)
    for s in range(2):
        d2d_copy(last, s).wait_send()
    for i in (last - 1, last):
        for t in range(finished(i)):
            fin_left(i, t)
    for i in range(len(CHUNKS)):
        for t in range(finished(i)):
            fin_there(i, t).wait_recv()
    for t in range(n_d - REST, n_d):
        rest_copy(t).wait()


def copy_kernel(src, dst, buf, in_sem, out_sem):
    rows = src.shape[0] // PIECES

    def load(p):
        at = pl.ds(p * rows, rows)
        return pltpu.make_async_copy(src.at[at, :], buf.at[at, :], in_sem.at[p])

    def store(p):
        at = pl.ds(p * rows, rows)
        return pltpu.make_async_copy(buf.at[at, :], dst.at[at, :], out_sem.at[p])

    for p in range(PIECES):
        load(p).start()
    for p in range(PIECES):
        load(p).wait()
        store(p).start()
    for p in range(PIECES):
        store(p).wait()


def place_kernel(y_in, here, there, y, sem):
    del y_in
    h, width = here.shape
    core = lax.rem(lax.axis_index("tp"), 2)
    copies = []
    for k, (src, half) in enumerate(((here, core), (there, 1 - core))):
        at = pl.multiple_of(y.shape[0] - 2 * h + half * h, h)
        copies.append(pltpu.make_async_copy(src, y.at[pl.ds(at, h), pl.ds(y.shape[1] - width, width)], sem.at[k]))
    for c in copies:
        c.start()
    for c in copies:
        c.wait()


def solution(mesh):
    def step(x, w_gate, w_up, w_down):
        (rows, depth), ff, width = x.shape, w_gate.shape[1], w_down.shape[1]
        big, n_d, n = max(CHUNKS), width // TD, len(CHUNKS)
        h = big // 2
        even, odd = max(CHUNKS[0::2]) // 2, max(CHUNKS[1::2]) // 2
        dma, vmem = pltpu.SemaphoreType.DMA, pltpu.VMEM
        anywhere = pl.BlockSpec(memory_space=pl.ANY)
        left = jax.ShapeDtypeStruct((CHUNKS[-1] // 2, REST * TD), BF16)
        whole = jax.ShapeDtypeStruct((rows, width), BF16)
        summed, rest = pl.pallas_call(
            kernel,
            out_shape=(whole, left),
            in_specs=[anywhere] * 4,
            out_specs=(anywhere, anywhere),
            scratch_shapes=[
                vmem((big, depth), BF16),
                vmem((big, ff), BF16),
                vmem((SLOTS, depth, 2 * TG), BF16),
                vmem((2, h, TD), F32),
                vmem((2, h, TD), BF16),
                vmem((2, h, TD), BF16),
                vmem((even, width), BF16),
                vmem((odd, width), BF16),
                vmem((even, width), BF16),
                vmem((odd, width), BF16),
                dma((4,)), dma((SLOTS, 2)), dma((2,)), dma((2,)), dma((2, n_d)), dma((2, n_d)),
                dma((2, n_d)), dma((2, n_d)), dma((n * n_d,)),
                pltpu.SemaphoreType.REGULAR, dma((REST,)),
            ],
            compiler_params=pltpu.CompilerParams(
                collective_id=0, has_side_effects=True, vmem_limit_bytes=66_900_000),
            cost_estimate=pl.CostEstimate(
                flops=6 * rows * depth * ff, bytes_accessed=n * 6 * depth * ff, transcendentals=rows * ff),
        )(x, w_gate, w_up, w_down)
        arrived = lax.ppermute(rest, "tp", [(i, (i + 2) % 4) for i in range(4)])
        result = pl.pallas_call(
            copy_kernel,
            out_shape=whole,
            in_specs=[anywhere],
            out_specs=anywhere,
            scratch_shapes=[vmem((rows, width), BF16), dma((PIECES,)), dma((PIECES,))],
            compiler_params=pltpu.CompilerParams(vmem_limit_bytes=40_000_000),
            cost_estimate=pl.CostEstimate(flops=COPY_COST, bytes_accessed=4 * rows * width, transcendentals=0),
        )(summed)
        arrived, result = lax.optimization_barrier((arrived, result))
        here = (rest.astype(F32) + arrived.astype(F32)).astype(BF16)
        there = lax.ppermute(here, "tp", [(i, i ^ 1) for i in range(4)])
        return pl.pallas_call(
            place_kernel,
            out_shape=whole,
            in_specs=[anywhere, pl.BlockSpec(memory_space=vmem), pl.BlockSpec(memory_space=vmem)],
            out_specs=anywhere,
            scratch_shapes=[dma((2,))],
            input_output_aliases={0: 0},
            compiler_params=pltpu.CompilerParams(vmem_limit_bytes=16_000_000),
        )(result, here, there)

    return jax.shard_map(
        step,
        mesh=mesh,
        in_specs=(P("dp", None), P(None, "tp"), P(None, "tp"), P("tp", None)),
        out_specs=P("dp", None),
        check_vma=False,
    )
```

```python
import functools

import jax
import jax.numpy as jnp
from jax import lax
from jax.experimental import pallas as pl
from jax.experimental.pallas import tpu as pltpu
from jax.sharding import PartitionSpec as P

CHUNKS = (512, 512, 448, 320, 256)
TG = 512
TD = 1024
SLOTS = 3
PIECES = 16
COPY_COST = 20_000_000_000
REST = 3
BF16, F32 = jnp.bfloat16, jnp.float32


def kernel(x, wg, wu, wd, y, rest, xb, hid, ring, own, snd, rcv, xs0, xs1, xr0, xr1,
           x_sem, ring_sem, d2d_s, d2d_r, ici_s, ici_r, fin_l, fin_s, fin_r, credit, rest_sem, half_sem):
    ff = wg.shape[1]
    n_gu, n_d = ff // TG, wd.shape[1] // TD
    per = n_gu + n_d
    last = len(CHUNKS) - 1
    first_row = [sum(CHUNKS[:i]) for i in range(len(CHUNKS))]
    xs, xr = (xs0, xs1), (xr0, xr1)
    me = lax.axis_index("tp")
    core = lax.rem(me, 2)
    partner = {"tp": me + 1 - 2 * core}
    across = {"tp": lax.rem(me + 2, 4)}
    remote = functools.partial(pltpu.make_async_remote_copy, device_id_type=pl.DeviceIdType.MESH)

    def block(j, width):
        return pl.ds(pl.multiple_of(j * width, width), width)

    def slot_of(i, s):
        return lax.rem(i * per + s, SLOTS)

    def g_copy(slot, j):
        return pltpu.make_async_copy(wg.at[:, block(j, TG)], ring.at[slot, :, pl.ds(0, TG)], ring_sem.at[slot, 0])

    def half_copy(w, at, k):
        cols = pl.ds(k * (TG // 2), TG // 2)
        return pltpu.make_async_copy(
            w.at[:, cols], ring.at[0, :, pl.ds(at * TG + k * (TG // 2), TG // 2)], half_sem.at[at, k])

    def u_copy(slot, j):
        return pltpu.make_async_copy(wu.at[:, block(j, TG)], ring.at[slot, :, pl.ds(TG, TG)], ring_sem.at[slot, 1])

    def d_copy(slot, j):
        return pltpu.make_async_copy(wd.at[:, block(j, TD)], ring.at[slot, pl.ds(0, ff), :], ring_sem.at[slot, 0])

    def x_copy(i, q):
        quarter = CHUNKS[i] // 4
        half = lax.rem(q // 2 + core, 2)
        at = pl.multiple_of(first_row[i] + (half * 2 + lax.rem(q, 2)) * quarter, quarter & -quarter)
        return pltpu.make_async_copy(x.at[pl.ds(at, quarter), :], xb.at[block(q, quarter), :], x_sem.at[q])

    def d2d_copy(i, s):
        h = CHUNKS[i] // 2
        return remote(snd.at[s, pl.ds(0, h), :], rcv.at[s, pl.ds(0, h), :], d2d_s.at[s], d2d_r.at[s], device_id=partner)

    def ici_copy(i, t):
        tile = (pl.ds(0, CHUNKS[i] // 2), block(t, TD))
        return remote(xs[i % 2].at[tile], xr[i % 2].at[tile], ici_s.at[i % 2, t], ici_r.at[i % 2, t], device_id=across)

    def fin_refs(i, t):
        h = CHUNKS[i] // 2
        at = pl.multiple_of(first_row[i] + core * h, h & -h)
        return xs[i % 2].at[pl.ds(0, h), block(t, TD)], y.at[pl.ds(at, h), block(t, TD)]

    def fin_here(i, t):
        src, dst = fin_refs(i, t)
        return pltpu.make_async_copy(src, dst, fin_l.at[i % 2, t])

    def fin_there(i, t):
        src, dst = fin_refs(i, t)
        return remote(src, dst, fin_s.at[i % 2, t], fin_r.at[i * n_d + t], device_id=partner)

    def fin_left(i, t):
        fin_here(i, t).wait()
        fin_there(i, t).wait_send()

    def rest_copy(t):
        k = t - (n_d - REST)
        src = xs[last % 2].at[pl.ds(0, CHUNKS[last] // 2), block(t, TD)]
        return pltpu.make_async_copy(src, rest.at[:, block(k, TD)], rest_sem.at[k])

    def reduce_tile(i, t):
        h, s = CHUNKS[i] // 2, lax.rem(i * n_d + t, 2)
        d2d_copy(i, s).wait_recv()
        if i >= 2:
            fin_left(i - 2, t)
        total = own[s, pl.ds(0, h), :] + rcv[s, pl.ds(0, h), :].astype(F32)
        xs[i % 2][pl.ds(0, h), block(t, TD)] = total.astype(BF16)
        if i < last:
            ici_copy(i, t).start()
        elif isinstance(t, int):
            rest_copy(t).start()
        else:
            pl.when(t < n_d - REST)(lambda: ici_copy(i, t).start())
            pl.when(t >= n_d - REST)(lambda: rest_copy(t).start())

    def finish_tile(i, t):
        copy = ici_copy(i, t)
        copy.wait_send()
        copy.wait_recv()
        tile = (pl.ds(0, CHUNKS[i] // 2), block(t, TD))
        total = xs[i % 2][tile].astype(F32) + xr[i % 2][tile].astype(F32)
        xs[i % 2][tile] = total.astype(BF16)
        fin_here(i, t).start()
        fin_there(i, t).start()

    for q in range(4):
        x_copy(0, q).start()
    half_copy(wg, 0, 0).start()
    half_copy(wu, 1, 0).start()

    barrier = pltpu.get_barrier_semaphore()
    for peer in (partner, across):
        pl.semaphore_signal(barrier, inc=1, device_id=peer, device_id_type=pl.DeviceIdType.MESH)
    pl.semaphore_wait(barrier, 2)

    for i, rows in enumerate(CHUNKS):
        h = rows // 2
        for q in range(4):
            x_copy(i, q).wait()

        def gate_up(slot, j, k):
            w = TG // 2
            gate = jnp.dot(xb[pl.ds(0, rows), :], ring[slot, :, pl.ds(k * w, w)], preferred_element_type=F32)
            up = jnp.dot(xb[pl.ds(0, rows), :], ring[slot, :, pl.ds(TG + k * w, w)], preferred_element_type=F32)
            act = gate * jax.nn.sigmoid(gate) * up
            hid[pl.ds(0, rows), pl.ds(pl.multiple_of(j * TG + k * w, w), w)] = act.astype(BF16)

        if i == 0:
            half_copy(wg, 0, 0).wait()
            half_copy(wu, 1, 0).wait()
            half_copy(wg, 0, 1).start()
            half_copy(wu, 1, 1).start()
            g_copy(1, 1).start()
            gate_up(0, 0, 0)
            half_copy(wg, 0, 1).wait()
            half_copy(wu, 1, 1).wait()
            u_copy(1, 1).start()
            g_copy(2, 2).start()
            u_copy(2, 2).start()
            gate_up(0, 0, 1)

        @pl.loop(1 if i == 0 else 0, n_gu)
        def _(j):
            slot, ahead, nxt = slot_of(i, j), slot_of(i, j + SLOTS - 1), j + SLOTS - 1
            g_copy(slot, j).wait()
            u_copy(slot, j).wait()

            @pl.when(nxt < n_gu)
            def _():
                g_copy(ahead, nxt).start()
                u_copy(ahead, nxt).start()

            @pl.when(nxt >= n_gu)
            def _():
                d_copy(ahead, nxt - n_gu).start()

            for k in range(2):
                gate_up(slot, j, k)

            if i > 0:

                @pl.when(j == 0)
                def _():
                    reduce_tile(i - 1, n_d - 1)

            if i > 1:

                @pl.when(j < n_d)
                def _():
                    finish_tile(i - 2, j)

                @pl.when(j == n_d - 1)
                def _():
                    pl.semaphore_signal(credit, inc=1, device_id=across, device_id_type=pl.DeviceIdType.MESH)

        @pl.loop(0, n_d)
        def _(j):
            slot, ahead, nxt = slot_of(i, n_gu + j), slot_of(i, n_gu + j + SLOTS - 1), j + SLOTS - 1
            s = lax.rem(i * n_d + j, 2)
            d_copy(slot, j).wait()

            @pl.when(nxt < n_d)
            def _():
                d_copy(ahead, nxt).start()

            if i < last:

                @pl.when(nxt >= n_d)
                def _():
                    g_copy(ahead, nxt - n_d).start()
                    u_copy(ahead, nxt - n_d).start()

                @pl.when(j < 4)
                def _():
                    x_copy(i + 1, j).start()

            @pl.when(j >= 2)
            def _():
                d2d_copy(i, s).wait_send()

            if i > 0:

                @pl.when(j < 2)
                def _():
                    d2d_copy(i - 1, s).wait_send()

            w = TD // 2
            for k in range(2):
                term = jnp.dot(hid[pl.ds(0, rows), :], ring[slot, pl.ds(0, ff), pl.ds(k * w, w)], preferred_element_type=F32)
                own[s, pl.ds(0, h), pl.ds(k * w, w)] = term[:h]
                snd[s, pl.ds(0, h), pl.ds(k * w, w)] = term[h:].astype(BF16)

            if 1 < i < last:

                @pl.when(j == 1)
                def _():
                    pl.semaphore_wait(credit, 1)

            @pl.when(j > (1 if i == last else 0))
            def _():
                reduce_tile(i, j - 1)

            d2d_copy(i, s).start()

            if i == last:

                @pl.when(j == 0)
                def _():
                    pl.semaphore_wait(credit, 1)
                    reduce_tile(i, j)

    reduce_tile(last, n_d - 1)
    def finished(i):
        return n_d if i < last else n_d - REST

    for i in (last - 1, last):
        for t in range(finished(i)):
            finish_tile(i, t)
    for s in range(2):
        d2d_copy(last, s).wait_send()
    for i in (last - 1, last):
        for t in range(finished(i)):
            fin_left(i, t)
    for i in range(len(CHUNKS)):
        for t in range(finished(i)):
            fin_there(i, t).wait_recv()
    for t in range(n_d - REST, n_d):
        rest_copy(t).wait()


def copy_kernel(src, dst, buf, in_sem, out_sem):
    rows = src.shape[0] // PIECES

    def load(p):
        at = pl.ds(p * rows, rows)
        return pltpu.make_async_copy(src.at[at, :], buf.at[at, :], in_sem.at[p])

    def store(p):
        at = pl.ds(p * rows, rows)
        return pltpu.make_async_copy(buf.at[at, :], dst.at[at, :], out_sem.at[p])

    for p in range(PIECES):
        load(p).start()
    for p in range(PIECES):
        load(p).wait()
        store(p).start()
    for p in range(PIECES):
        store(p).wait()


def place_kernel(y_in, here, there, y, sem):
    del y_in
    h, width = here.shape
    core = lax.rem(lax.axis_index("tp"), 2)
    copies = []
    for k, (src, half) in enumerate(((here, core), (there, 1 - core))):
        at = pl.multiple_of(y.shape[0] - 2 * h + half * h, h)
        copies.append(pltpu.make_async_copy(src, y.at[pl.ds(at, h), pl.ds(y.shape[1] - width, width)], sem.at[k]))
    for c in copies:
        c.start()
    for c in copies:
        c.wait()


def solution(mesh):
    def step(x, w_gate, w_up, w_down):
        (rows, depth), ff, width = x.shape, w_gate.shape[1], w_down.shape[1]
        big, n_d, n = max(CHUNKS), width // TD, len(CHUNKS)
        h = big // 2
        even, odd = max(CHUNKS[0::2]) // 2, max(CHUNKS[1::2]) // 2
        dma, vmem = pltpu.SemaphoreType.DMA, pltpu.VMEM
        anywhere = pl.BlockSpec(memory_space=pl.ANY)
        left = jax.ShapeDtypeStruct((CHUNKS[-1] // 2, REST * TD), BF16)
        whole = jax.ShapeDtypeStruct((rows, width), BF16)
        summed, rest = pl.pallas_call(
            kernel,
            out_shape=(whole, left),
            in_specs=[anywhere] * 4,
            out_specs=(anywhere, anywhere),
            scratch_shapes=[
                vmem((big, depth), BF16),
                vmem((big, ff), BF16),
                vmem((SLOTS, depth, 2 * TG), BF16),
                vmem((2, h, TD), F32),
                vmem((2, h, TD), BF16),
                vmem((2, h, TD), BF16),
                vmem((even, width), BF16),
                vmem((odd, width), BF16),
                vmem((even, width), BF16),
                vmem((odd, width), BF16),
                dma((4,)), dma((SLOTS, 2)), dma((2,)), dma((2,)), dma((2, n_d)), dma((2, n_d)),
                dma((2, n_d)), dma((2, n_d)), dma((n * n_d,)),
                pltpu.SemaphoreType.REGULAR, dma((REST,)), dma((2, 2)),
            ],
            compiler_params=pltpu.CompilerParams(
                collective_id=0, has_side_effects=True, vmem_limit_bytes=66_900_000),
            cost_estimate=pl.CostEstimate(
                flops=6 * rows * depth * ff, bytes_accessed=n * 6 * depth * ff, transcendentals=rows * ff),
        )(x, w_gate, w_up, w_down)
        arrived = lax.ppermute(rest, "tp", [(i, (i + 2) % 4) for i in range(4)])
        result = pl.pallas_call(
            copy_kernel,
            out_shape=whole,
            in_specs=[anywhere],
            out_specs=anywhere,
            scratch_shapes=[vmem((rows, width), BF16), dma((PIECES,)), dma((PIECES,))],
            compiler_params=pltpu.CompilerParams(vmem_limit_bytes=40_000_000),
            cost_estimate=pl.CostEstimate(flops=COPY_COST, bytes_accessed=4 * rows * width, transcendentals=0),
        )(summed)
        arrived, result = lax.optimization_barrier((arrived, result))
        here = (rest.astype(F32) + arrived.astype(F32)).astype(BF16)
        there = lax.ppermute(here, "tp", [(i, i ^ 1) for i in range(4)])
        return pl.pallas_call(
            place_kernel,
            out_shape=whole,
            in_specs=[anywhere, pl.BlockSpec(memory_space=vmem), pl.BlockSpec(memory_space=vmem)],
            out_specs=anywhere,
            scratch_shapes=[dma((2,))],
            input_output_aliases={0: 0},
            compiler_params=pltpu.CompilerParams(vmem_limit_bytes=16_000_000),
        )(result, here, there)

    return jax.shard_map(
        step,
        mesh=mesh,
        in_specs=(P("dp", None), P(None, "tp"), P(None, "tp"), P("tp", None)),
        out_specs=P("dp", None),
        check_vma=False,
    )
```

```python
import functools

import jax
import jax.numpy as jnp
from jax import lax
from jax.experimental import pallas as pl
from jax.experimental.pallas import tpu as pltpu
from jax.sharding import PartitionSpec as P

CHUNKS = (512, 512, 448, 320, 256)
TG = 512
TD = 1024
SLOTS = 3
PIECES = 16
COPY_COST = 20_000_000_000
REST = 3
BF16, F32 = jnp.bfloat16, jnp.float32


def kernel(x, wg, wu, wd, y, rest, xb, hid, ring, own, snd, rcv, xs0, xs1, xr0, xr1,
           x_sem, ring_sem, d2d_s, d2d_r, ici_s, ici_r, fin_l, fin_s, fin_r, credit, rest_sem, half_sem):
    ff = wg.shape[1]
    n_gu, n_d = ff // TG, wd.shape[1] // TD
    per = n_gu + n_d
    last = len(CHUNKS) - 1
    first_row = [sum(CHUNKS[:i]) for i in range(len(CHUNKS))]
    xs, xr = (xs0, xs1), (xr0, xr1)
    me = lax.axis_index("tp")
    core = lax.rem(me, 2)
    partner = {"tp": me + 1 - 2 * core}
    across = {"tp": lax.rem(me + 2, 4)}
    remote = functools.partial(pltpu.make_async_remote_copy, device_id_type=pl.DeviceIdType.MESH)

    def block(j, width):
        return pl.ds(pl.multiple_of(j * width, width), width)

    def slot_of(i, s):
        return lax.rem(i * per + s, SLOTS)

    def g_copy(slot, j):
        return pltpu.make_async_copy(wg.at[:, block(j, TG)], ring.at[slot, :, pl.ds(0, TG)], ring_sem.at[slot, 0])

    def half_copy(w, at, k):
        cols = pl.ds(k * (TG // 2), TG // 2)
        return pltpu.make_async_copy(
            w.at[:, cols], ring.at[0, :, pl.ds(at * TG + k * (TG // 2), TG // 2)], half_sem.at[at, k])

    def u_copy(slot, j):
        return pltpu.make_async_copy(wu.at[:, block(j, TG)], ring.at[slot, :, pl.ds(TG, TG)], ring_sem.at[slot, 1])

    def d_copy(slot, j):
        return pltpu.make_async_copy(wd.at[:, block(j, TD)], ring.at[slot, pl.ds(0, ff), :], ring_sem.at[slot, 0])

    def x_copy(i, q):
        quarter = CHUNKS[i] // 4
        half = lax.rem(q // 2 + core, 2)
        at = pl.multiple_of(first_row[i] + (half * 2 + lax.rem(q, 2)) * quarter, quarter & -quarter)
        return pltpu.make_async_copy(x.at[pl.ds(at, quarter), :], xb.at[block(q, quarter), :], x_sem.at[q])

    def d2d_copy(i, s):
        h = CHUNKS[i] // 2
        return remote(snd.at[s, pl.ds(0, h), :], rcv.at[s, pl.ds(0, h), :], d2d_s.at[s], d2d_r.at[s], device_id=partner)

    def ici_copy(i, t):
        tile = (pl.ds(0, CHUNKS[i] // 2), block(t, TD))
        return remote(xs[i % 2].at[tile], xr[i % 2].at[tile], ici_s.at[i % 2, t], ici_r.at[i % 2, t], device_id=across)

    def fin_refs(i, t):
        h = CHUNKS[i] // 2
        at = pl.multiple_of(first_row[i] + core * h, h & -h)
        return xs[i % 2].at[pl.ds(0, h), block(t, TD)], y.at[pl.ds(at, h), block(t, TD)]

    def fin_here(i, t):
        src, dst = fin_refs(i, t)
        return pltpu.make_async_copy(src, dst, fin_l.at[i % 2, t])

    def fin_there(i, t):
        src, dst = fin_refs(i, t)
        return remote(src, dst, fin_s.at[i % 2, t], fin_r.at[i * n_d + t], device_id=partner)

    def fin_left(i, t):
        fin_here(i, t).wait()
        fin_there(i, t).wait_send()

    def rest_copy(t):
        k = t - (n_d - REST)
        src = xs[last % 2].at[pl.ds(0, CHUNKS[last] // 2), block(t, TD)]
        return pltpu.make_async_copy(src, rest.at[:, block(k, TD)], rest_sem.at[k])

    def reduce_tile(i, t):
        h, s = CHUNKS[i] // 2, lax.rem(i * n_d + t, 2)
        d2d_copy(i, s).wait_recv()
        if i >= 2:
            fin_left(i - 2, t)
        total = own[s, pl.ds(0, h), :] + rcv[s, pl.ds(0, h), :].astype(F32)
        xs[i % 2][pl.ds(0, h), block(t, TD)] = total.astype(BF16)
        if i < last:
            ici_copy(i, t).start()
        elif isinstance(t, int):
            rest_copy(t).start()
        else:
            pl.when(t < n_d - REST)(lambda: ici_copy(i, t).start())
            pl.when(t >= n_d - REST)(lambda: rest_copy(t).start())

    def finish_tile(i, t):
        copy = ici_copy(i, t)
        copy.wait_send()
        copy.wait_recv()
        tile = (pl.ds(0, CHUNKS[i] // 2), block(t, TD))
        total = xs[i % 2][tile].astype(F32) + xr[i % 2][tile].astype(F32)
        xs[i % 2][tile] = total.astype(BF16)
        fin_here(i, t).start()
        fin_there(i, t).start()

    for q in range(4):
        x_copy(0, q).start()
    half_copy(wg, 0, 0).start()
    half_copy(wu, 1, 0).start()

    barrier = pltpu.get_barrier_semaphore()
    for peer in (partner, across):
        pl.semaphore_signal(barrier, inc=1, device_id=peer, device_id_type=pl.DeviceIdType.MESH)
    pl.semaphore_wait(barrier, 2)

    for i, rows in enumerate(CHUNKS):
        h = rows // 2
        for q in range(4):
            x_copy(i, q).wait()

        def gate_up(slot, j, k):
            w = TG // 2
            gate = jnp.dot(xb[pl.ds(0, rows), :], ring[slot, :, pl.ds(k * w, w)], preferred_element_type=F32)
            up = jnp.dot(xb[pl.ds(0, rows), :], ring[slot, :, pl.ds(TG + k * w, w)], preferred_element_type=F32)
            act = gate * jax.nn.sigmoid(gate) * up
            hid[pl.ds(0, rows), pl.ds(pl.multiple_of(j * TG + k * w, w), w)] = act.astype(BF16)

        if i == 0:
            half_copy(wg, 0, 0).wait()
            half_copy(wu, 1, 0).wait()
            half_copy(wg, 0, 1).start()
            half_copy(wu, 1, 1).start()
            g_copy(1, 1).start()
            gate_up(0, 0, 0)
            half_copy(wg, 0, 1).wait()
            half_copy(wu, 1, 1).wait()
            u_copy(1, 1).start()
            for early in range(2, SLOTS):
                g_copy(early, early).start()
                u_copy(early, early).start()
            gate_up(0, 0, 1)

        @pl.loop(1 if i == 0 else 0, n_gu)
        def _(j):
            slot, ahead, nxt = slot_of(i, j), slot_of(i, j + SLOTS - 1), j + SLOTS - 1
            g_copy(slot, j).wait()
            u_copy(slot, j).wait()

            @pl.when(nxt < n_gu)
            def _():
                g_copy(ahead, nxt).start()
                u_copy(ahead, nxt).start()

            @pl.when(nxt >= n_gu)
            def _():
                d_copy(ahead, nxt - n_gu).start()

            for k in range(2):
                gate_up(slot, j, k)

            if i > 0:

                @pl.when(j == 0)
                def _():
                    reduce_tile(i - 1, n_d - 1)

            if i > 1:

                @pl.when(j < n_d)
                def _():
                    finish_tile(i - 2, j)

                @pl.when(j == n_d - 1)
                def _():
                    pl.semaphore_signal(credit, inc=1, device_id=across, device_id_type=pl.DeviceIdType.MESH)

        @pl.loop(0, n_d)
        def _(j):
            slot, ahead, nxt = slot_of(i, n_gu + j), slot_of(i, n_gu + j + SLOTS - 1), j + SLOTS - 1
            s = lax.rem(i * n_d + j, 2)
            d_copy(slot, j).wait()

            @pl.when(nxt < n_d)
            def _():
                d_copy(ahead, nxt).start()

            if i < last:

                @pl.when(nxt >= n_d)
                def _():
                    g_copy(ahead, nxt - n_d).start()
                    u_copy(ahead, nxt - n_d).start()

                @pl.when(j < 4)
                def _():
                    x_copy(i + 1, j).start()

            @pl.when(j >= 2)
            def _():
                d2d_copy(i, s).wait_send()

            if i > 0:

                @pl.when(j < 2)
                def _():
                    d2d_copy(i - 1, s).wait_send()

            w = TD // 2
            for k in range(2):
                term = jnp.dot(hid[pl.ds(0, rows), :], ring[slot, pl.ds(0, ff), pl.ds(k * w, w)], preferred_element_type=F32)
                own[s, pl.ds(0, h), pl.ds(k * w, w)] = term[:h]
                snd[s, pl.ds(0, h), pl.ds(k * w, w)] = term[h:].astype(BF16)

            if 1 < i < last:

                @pl.when(j == 1)
                def _():
                    pl.semaphore_wait(credit, 1)

            @pl.when(j > (1 if i == last else 0))
            def _():
                reduce_tile(i, j - 1)

            d2d_copy(i, s).start()

            if i == last:

                @pl.when(j == 0)
                def _():
                    pl.semaphore_wait(credit, 1)
                    reduce_tile(i, j)

    reduce_tile(last, n_d - 1)
    def finished(i):
        return n_d if i < last else n_d - REST

    for i in (last - 1, last):
        for t in range(finished(i)):
            finish_tile(i, t)
    for s in range(2):
        d2d_copy(last, s).wait_send()
    for i in (last - 1, last):
        for t in range(finished(i)):
            fin_left(i, t)
    for i in range(len(CHUNKS)):
        for t in range(finished(i)):
            fin_there(i, t).wait_recv()
    for t in range(n_d - REST, n_d):
        rest_copy(t).wait()


def copy_kernel(src, dst, buf, in_sem, out_sem):
    rows = src.shape[0] // PIECES

    def load(p):
        at = pl.ds(p * rows, rows)
        return pltpu.make_async_copy(src.at[at, :], buf.at[at, :], in_sem.at[p])

    def store(p):
        at = pl.ds(p * rows, rows)
        return pltpu.make_async_copy(buf.at[at, :], dst.at[at, :], out_sem.at[p])

    for p in range(PIECES):
        load(p).start()
    for p in range(PIECES):
        load(p).wait()
        store(p).start()
    for p in range(PIECES):
        store(p).wait()


def place_kernel(y_in, here, there, y, sem):
    del y_in
    h, width = here.shape
    core = lax.rem(lax.axis_index("tp"), 2)
    copies = []
    for k, (src, half) in enumerate(((here, core), (there, 1 - core))):
        at = pl.multiple_of(y.shape[0] - 2 * h + half * h, h)
        copies.append(pltpu.make_async_copy(src, y.at[pl.ds(at, h), pl.ds(y.shape[1] - width, width)], sem.at[k]))
    for c in copies:
        c.start()
    for c in copies:
        c.wait()


def solution(mesh):
    def step(x, w_gate, w_up, w_down):
        (rows, depth), ff, width = x.shape, w_gate.shape[1], w_down.shape[1]
        big, n_d, n = max(CHUNKS), width // TD, len(CHUNKS)
        h = big // 2
        even, odd = max(CHUNKS[0::2]) // 2, max(CHUNKS[1::2]) // 2
        dma, vmem = pltpu.SemaphoreType.DMA, pltpu.VMEM
        anywhere = pl.BlockSpec(memory_space=pl.ANY)
        left = jax.ShapeDtypeStruct((CHUNKS[-1] // 2, REST * TD), BF16)
        whole = jax.ShapeDtypeStruct((rows, width), BF16)
        summed, rest = pl.pallas_call(
            kernel,
            out_shape=(whole, left),
            in_specs=[anywhere] * 4,
            out_specs=(anywhere, anywhere),
            scratch_shapes=[
                vmem((big, depth), BF16),
                vmem((big, ff), BF16),
                vmem((SLOTS, depth, 2 * TG), BF16),
                vmem((2, h, TD), F32),
                vmem((2, h, TD), BF16),
                vmem((2, h, TD), BF16),
                vmem((even, width), BF16),
                vmem((odd, width), BF16),
                vmem((even, width), BF16),
                vmem((odd, width), BF16),
                dma((4,)), dma((SLOTS, 2)), dma((2,)), dma((2,)), dma((2, n_d)), dma((2, n_d)),
                dma((2, n_d)), dma((2, n_d)), dma((n * n_d,)),
                pltpu.SemaphoreType.REGULAR, dma((REST,)), dma((2, 2)),
            ],
            compiler_params=pltpu.CompilerParams(
                collective_id=0, has_side_effects=True, vmem_limit_bytes=66_900_000),
            cost_estimate=pl.CostEstimate(
                flops=6 * rows * depth * ff, bytes_accessed=n * 6 * depth * ff, transcendentals=rows * ff),
        )(x, w_gate, w_up, w_down)
        arrived = lax.ppermute(rest, "tp", [(i, (i + 2) % 4) for i in range(4)])
        result = pl.pallas_call(
            copy_kernel,
            out_shape=whole,
            in_specs=[anywhere],
            out_specs=anywhere,
            scratch_shapes=[vmem((rows, width), BF16), dma((PIECES,)), dma((PIECES,))],
            compiler_params=pltpu.CompilerParams(vmem_limit_bytes=40_000_000),
            cost_estimate=pl.CostEstimate(flops=COPY_COST, bytes_accessed=4 * rows * width, transcendentals=0),
        )(summed)
        arrived, result = lax.optimization_barrier((arrived, result))
        here = (rest.astype(F32) + arrived.astype(F32)).astype(BF16)
        there = lax.ppermute(here, "tp", [(i, i ^ 1) for i in range(4)])
        return pl.pallas_call(
            place_kernel,
            out_shape=whole,
            in_specs=[anywhere, pl.BlockSpec(memory_space=vmem), pl.BlockSpec(memory_space=vmem)],
            out_specs=anywhere,
            scratch_shapes=[dma((2,))],
            input_output_aliases={0: 0},
            compiler_params=pltpu.CompilerParams(vmem_limit_bytes=16_000_000),
        )(result, here, there)

    return jax.shard_map(
        step,
        mesh=mesh,
        in_specs=(P("dp", None), P(None, "tp"), P(None, "tp"), P("tp", None)),
        out_specs=P("dp", None),
        check_vma=False,
    )
```
